32 devices in a mesh: mp: 4 (over z), dp: 8 (over y, x, core).
Axes of the slice: x: 2, y: 2, z: 4, core: 2. Of those that a mesh axis runs over, the one named last changes fastest.
Arguments:
- a_mat: bfloat16 [3072, 196608], P(('mp', 'dp'))
- b_mat: bfloat16 [196608, 768], P(('mp', 'dp'))
Outputs:
- output: bfloat16 [3072, 768], P(('mp', 'dp'))
All inputs are finite; a program needn't handle non-finite values.
Results may differ from the reference program's by a relative error of at most 0.001.
Values are sent between devices in bfloat16 or wider.
A program may use at most 1 GiB of HBM per device.

```python
import jax
import jax.numpy as jnp

M_DIM = 3072
N_DIM = 768
TOKENS = 196608


def setup_inputs(seed: int = 0) -> dict:
    root_key = jax.random.key(seed)
    key_a, key_b = jax.random.split(root_key)
    a_mat = jax.random.normal(key_a, (M_DIM, TOKENS), jnp.float32)
    b_mat = jax.random.normal(key_b, (TOKENS, N_DIM), jnp.float32) * (TOKENS ** -0.5)
    return {"a_mat": a_mat.astype(jnp.bfloat16), "b_mat": b_mat.astype(jnp.bfloat16)}


def reference(a_mat, b_mat):
    return jnp.dot(a_mat, b_mat, preferred_element_type=jnp.float32).astype(jnp.bfloat16)
```

```python
import functools

import jax
import jax.numpy as jnp
from jax import lax
from jax.experimental import pallas as pl
from jax.experimental.pallas import tpu as pltpu
from jax.sharding import PartitionSpec as P

MESH = pl.DeviceIdType.MESH
CHUNKS = 24
AHEAD = 3
STOCK = 3


def mask_bits(pos):
    return (pos >> 1) & 1, pos & 1, pos >> 2


def flip(bit, by):
    return 1 - bit if by else bit


def kernel(
    n, a_ref, b_ref, c_ref, ra, rx, r0, r1, fa,
    acc, acc2, va, vb, core_in, plane_in, core_in2, plane_in2, back,
    send_a, recv_a, send_o, recv_o, send_x, recv_x, load_sem, rs_send, rs_recv, back_sem,
):
    z, dp = lax.axis_index("mp"), lax.axis_index("dp")
    y, x, core = dp // 4, (dp // 2) % 2, dp % 2
    rows = a_ref.shape[0]
    tok = b_ref.shape[0]
    kc = tok // n
    slots = 2 * n
    high = z // 2
    is_mid = ((z + 1) // 2) % 2 == 1
    is_end = jnp.logical_not(is_mid)
    pair = (z // 2) * 2 + (1 - z % 2)
    across = 3 - z
    peers = []
    for pos in range(1, 8):
        my, mx, mc = mask_bits(pos)
        peers.append(flip(y, my) * 4 + flip(x, mx) * 2 + flip(core, mc))

    def block_of(near):
        return near + high * (3 - 2 * near)

    def a_cols(u, w, owner):
        phase = u // n
        near = 2 + phase if w else 1 - phase
        start = (block_of(near) * 8 + owner) * tok + (u % n) * kc
        return pl.ds(pl.multiple_of(start, kc), kc)

    def at(i):
        return pl.ds(pl.multiple_of(i * kc, kc), kc)

    def a_send(u, w, pos):
        return pltpu.make_async_remote_copy(
            src_ref=a_ref.at[:, a_cols(u, w, peers[pos - 1])],
            dst_ref=ra.at[w, pl.ds((pos - 1) * rows, rows), at(u)],
            send_sem=send_a.at[u],
            recv_sem=recv_a.at[u],
            device_id=(z, peers[pos - 1]),
            device_id_type=MESH,
        )

    def exchange_a(u):
        for w in range(2):
            for pos in (3, 7, 1, 2, 5, 6, 4):
                a_send(u, w, pos).start()

    def wait(ref, sem):
        pltpu.make_async_copy(ref, ref, sem).wait()

    def wait_sent_a(u):
        wait(ra.at[:, :, at(u)], send_a.at[u])

    def to_pair(src, dst, slot):
        return pltpu.make_async_remote_copy(
            src_ref=src, dst_ref=dst, send_sem=send_o.at[slot], recv_sem=recv_o.at[slot],
            device_id=(pair, dp), device_id_type=MESH,
        )

    def to_across(src, u):
        return pltpu.make_async_remote_copy(
            src_ref=src, dst_ref=rx.at[at(u)], send_sem=send_x.at[u], recv_sem=recv_x.at[u],
            device_id=(across, dp), device_id_type=MESH,
        )

    @pl.when(is_mid)
    def _():
        to_across(b_ref.at[at(0)], 0).start()
        to_pair(b_ref.at[at(0)], r1, 0).start()
        to_across(b_ref.at[at(1)], 1).start()

    @pl.when(is_end)
    def _():
        for j in range(STOCK):
            to_pair(b_ref.at[at(j)], r0.at[at(j)], j).start()

    for u in range(AHEAD):
        exchange_a(u)

    acc[...] = jnp.zeros_like(acc)
    acc2[...] = jnp.zeros_like(acc2)

    def load_a(u, w, slot):
        own = pltpu.make_async_copy(
            a_ref.at[:, a_cols(u, w, dp)], va.at[slot, pl.ds(0, rows)], load_sem.at[slot, 0]
        )
        others = pltpu.make_async_copy(
            ra.at[w, :, at(u)], va.at[slot, pl.ds(rows, 7 * rows)], load_sem.at[slot, 1]
        )
        own.start()
        others.start()

    def load_fa(i, slot):
        pltpu.make_async_copy(fa.at[:, at(i)], va.at[slot], load_sem.at[slot, 0]).start()

    def load_b(src, slot):
        pltpu.make_async_copy(src, vb.at[slot], load_sem.at[slot, 2]).start()

    def product(total, slot):
        size = (8 * rows) // 4

        def part(r, carry):
            at_r = pl.ds(pl.multiple_of(r * size, size), size)
            total[at_r] += jnp.dot(va[slot, at_r], vb[slot], preferred_element_type=jnp.float32)
            return carry

        lax.fori_loop(0, 4, part, 0)

    def core_step(total, landing, k):
        my = flip(core, 1)
        return pltpu.make_async_remote_copy(
            src_ref=total.at[pl.ds(4 * rows, 4 * rows)], dst_ref=landing,
            send_sem=rs_send.at[k, 0], recv_sem=rs_recv.at[k, 0],
            device_id=(z, y * 4 + x * 2 + my), device_id_type=MESH,
        )

    def plane_step(total, landing, k, pos):
        return pltpu.make_async_remote_copy(
            src_ref=total.at[pl.ds(pos * rows, rows)], dst_ref=landing.at[pos - 1],
            send_sem=rs_send.at[k, pos], recv_sem=rs_recv.at[k, pos],
            device_id=(z, peers[pos - 1]), device_id_type=MESH,
        )

    def step(t, carry):
        @pl.when(is_mid)
        def _():
            @pl.when(t < slots)
            def _():
                wait(rx.at[at(t)], recv_x.at[t])
                to_pair(rx.at[at(t)], rx.at[at(t)], t + 1).start()

            @pl.when(t < slots - 1)
            def _():
                wait(r0.at[at(0)], recv_o.at[t])

            @pl.when(jnp.logical_and(t >= n - 1, t < slots - 1))
            def _():
                to_across(r0.at[at(t - n + 1)], t + 1).start()

            @pl.when(t + 2 < n)
            def _():
                to_across(b_ref.at[at(t + 2)], t + 2).start()

        @pl.when(is_end)
        def _():
            wait(r1, recv_o.at[t])

            @pl.when(jnp.logical_and(t >= STOCK + n - 2, t < slots - 2))
            def _():
                j = t - n + 2
                to_pair(b_ref.at[at(j)], r0.at[at(j)], t + 1).start()

        u = t - 1

        @pl.when(t >= 1)
        def _():
            wait(ra.at[:, :, at(u)], recv_a.at[u])

        @pl.when(jnp.logical_and(is_end, jnp.logical_and(t + 1 >= STOCK, t + 1 < STOCK + n - 1)))
        def _():
            i = t + 2 - STOCK
            to_pair(a_ref.at[:, a_cols(i, 0, dp)], fa.at[pl.ds(0, rows), at(i)], t + 1).start()
            to_pair(ra.at[0, :, at(i)], fa.at[pl.ds(rows, 7 * rows), at(i)], t + 1).start()

        @pl.when(t + AHEAD < slots)
        def _():
            wait_sent_a(t)
            exchange_a(t + AHEAD)

        first = jnp.logical_and(t >= 1, jnp.logical_or(is_mid, jnp.logical_or(t == 1, u >= n)))
        third = jnp.logical_and(is_mid, jnp.logical_and(t >= STOCK, t < STOCK + n - 1))

        @pl.when(t >= 1)
        def _():
            load_a(u, 1, 1)
            load_b(rx.at[at(u)], 1)

        @pl.when(first)
        def _():
            load_a(u, 0, 0)

            @pl.when(is_mid)
            def _():
                @pl.when(u < n)
                def _():
                    load_b(b_ref.at[at(u)], 0)

                @pl.when(u >= n)
                def _():
                    load_b(r0.at[at(u - n)], 0)

            @pl.when(is_end)
            def _():
                @pl.when(u < n)
                def _():
                    load_b(r1, 0)

                @pl.when(u >= n)
                def _():
                    load_b(b_ref.at[at(u - n)], 0)

        @pl.when(third)
        def _():
            i = t - STOCK + 1
            load_fa(i, 2)
            load_b(b_ref.at[at(i)], 2)

        def wait_load(slot, parts):
            if parts == 3:
                wait(va.at[slot, pl.ds(0, rows)], load_sem.at[slot, 0])
                wait(va.at[slot, pl.ds(rows, 7 * rows)], load_sem.at[slot, 1])
            else:
                wait(va.at[slot], load_sem.at[slot, 0])
            wait(vb.at[slot], load_sem.at[slot, 2])

        @pl.when(first)
        def _():
            wait_load(0, 3)
            product(acc, 0)

        @pl.when(third)
        def _():
            wait_load(2, 2)
            product(acc2, 2)

        @pl.when(t >= 1)
        def _():
            wait_load(1, 3)
            product(acc, 1)

        done = STOCK + n - 2

        @pl.when(jnp.logical_and(is_mid, t == done + 1))
        def _():
            core_step(acc2, core_in2, 0).start()

        @pl.when(jnp.logical_and(is_mid, t == done + 2))
        def _():
            core_step(acc2, core_in2, 0).wait()
            acc2[pl.ds(0, 4 * rows)] += core_in2[...]

        @pl.when(jnp.logical_and(is_mid, t == done + 3))
        def _():
            for pos in (3, 1, 2):
                plane_step(acc2, plane_in2, 0, pos).start()

        @pl.when(jnp.logical_and(is_mid, t == done + 6))
        def _():
            for pos in (3, 1, 2):
                plane_step(acc2, plane_in2, 0, pos).wait()
            acc2[pl.ds(0, rows)] += (plane_in2[0] + plane_in2[1]) + plane_in2[2]

        return carry

    lax.fori_loop(0, slots + 1, step, 0)

    core_copy = core_step(acc, core_in, 1)
    core_copy.start()
    back_copy = pltpu.make_async_remote_copy(
        src_ref=acc2.at[pl.ds(0, rows)], dst_ref=back, send_sem=back_sem.at[0], recv_sem=back_sem.at[1],
        device_id=(pair, dp), device_id_type=MESH,
    )

    @pl.when(is_mid)
    def _():
        back_copy.start()

    core_copy.wait()
    acc[pl.ds(rows, 3 * rows)] += core_in[pl.ds(rows, 3 * rows)]
    plane_copies = [plane_step(acc, plane_in, 1, pos) for pos in (3, 1, 2)]
    for copy in plane_copies:
        copy.start()
    total = acc[pl.ds(0, rows)] + core_in[pl.ds(0, rows)]

    def sent_a(u, carry):
        wait_sent_a(u)
        return carry

    lax.fori_loop(slots - AHEAD, slots, sent_a, 0)

    @pl.when(is_mid)
    def _():
        def sent(s, carry):
            wait(rx.at[at(0)], send_x.at[s])
            return carry

        lax.fori_loop(0, slots, sent, 0)

        def sent_o(s, carry):
            wait(rx.at[at(0)], send_o.at[s])
            return carry

        lax.fori_loop(0, slots + 1, sent_o, 0)

    @pl.when(is_end)
    def _():
        def sent_o(s, carry):
            wait(rx.at[at(0)], send_o.at[s])
            return carry

        lax.fori_loop(0, slots - 1, sent_o, 0)

    for copy in plane_copies:
        copy.wait()
    total += (plane_in[0] + plane_in[1]) + plane_in[2]

    @pl.when(is_mid)
    def _():
        back_copy.wait_send()
        c_ref[...] = total.astype(c_ref.dtype)

    @pl.when(is_end)
    def _():
        back_copy.wait_recv()
        c_ref[...] = (total + back[...]).astype(c_ref.dtype)


def solution(mesh):
    n = CHUNKS

    def local_product(a_rows, b_rows):
        rows, tok, cols = a_rows.shape[0], b_rows.shape[0], b_rows.shape[1]
        kc = tok // n
        slots = 2 * n
        bf16, f32 = jnp.bfloat16, jnp.float32
        hbm = pl.BlockSpec(memory_space=pltpu.HBM)
        out = pl.pallas_call(
            functools.partial(kernel, n),
            name="product",
            out_shape=(
                jax.ShapeDtypeStruct((rows, cols), bf16),
                jax.ShapeDtypeStruct((2, 7 * rows, 2 * tok), bf16),
                jax.ShapeDtypeStruct((2 * tok, cols), bf16),
                jax.ShapeDtypeStruct((tok, cols), bf16),
                jax.ShapeDtypeStruct((kc, cols), bf16),
                jax.ShapeDtypeStruct((8 * rows, tok), bf16),
            ),
            in_specs=[hbm, hbm],
            out_specs=(pl.BlockSpec(memory_space=pltpu.VMEM), hbm, hbm, hbm, hbm, hbm),
            scratch_shapes=[
                pltpu.VMEM((8 * rows, cols), f32),
                pltpu.VMEM((8 * rows, cols), f32),
                pltpu.VMEM((3, 8 * rows, kc), bf16),
                pltpu.VMEM((3, kc, cols), bf16),
                pltpu.VMEM((4 * rows, cols), f32),
                pltpu.VMEM((3, rows, cols), f32),
                pltpu.VMEM((4 * rows, cols), f32),
                pltpu.VMEM((3, rows, cols), f32),
                pltpu.VMEM((rows, cols), f32),
                pltpu.SemaphoreType.DMA((slots,)),
                pltpu.SemaphoreType.DMA((slots,)),
                pltpu.SemaphoreType.DMA((slots + 1,)),
                pltpu.SemaphoreType.DMA((slots + 1,)),
                pltpu.SemaphoreType.DMA((slots,)),
                pltpu.SemaphoreType.DMA((slots,)),
                pltpu.SemaphoreType.DMA((3, 3)),
                pltpu.SemaphoreType.DMA((2, 4)),
                pltpu.SemaphoreType.DMA((2, 4)),
                pltpu.SemaphoreType.DMA((2,)),
            ],
            compiler_params=pltpu.CompilerParams(has_side_effects=True),
        )(a_rows, b_rows)
        return out[0]

    return jax.shard_map(
        local_product,
        mesh=mesh,
        in_specs=(P(("mp", "dp"), None), P(("mp", "dp"), None)),
        out_specs=P(("mp", "dp"), None),
        check_vma=False,
    )
```
